8 devices in a mesh: data: 1 (over z), outer: 2 (over y), expert: 4 (over x, core).
Axes of the slice: x: 2, y: 2, z: 1, core: 2. Of those that a mesh axis runs over, the one named last changes fastest.
Arguments:
- tokens: bfloat16 [2048, 1536], P(('data', 'outer', 'expert'))
- w_router: bfloat16 [1536, 40], replicated
- routes: int32 [2048, 8], P(('data', 'outer', 'expert'))
- w_gate: bfloat16 [40, 1536, 512], P(('outer', 'expert'))
- w_up: bfloat16 [40, 1536, 512], P(('outer', 'expert'))
- w_down: bfloat16 [40, 512, 1536], P(('outer', 'expert'))
Outputs:
- output: bfloat16 [2048, 1536], P(('data', 'outer', 'expert'))
All inputs are finite; a program needn't handle non-finite values.
Results may differ from the reference program's by a relative error of at most 0.001.
Values are sent between devices in bfloat16 or wider.
A program may use at most 1 GiB of HBM per device.

```python
import jax
import jax.numpy as jnp
from jax import lax

D = 1536
FF = 512
EXPERTS = 40
TOPK = 8
TOKENS = 256
OUTER = 2
GROUP = 4
LIMIT = 1

DEVICES = OUTER * GROUP
ROWS = DEVICES * TOKENS
PER_OUTER = EXPERTS // OUTER
CAPACITY = (5 * TOKENS * TOPK + 4 * EXPERTS - 1) // (4 * EXPERTS)


def draw_routes(route_key):
    key_hot, key_grp, key_exp = jax.random.split(route_key, 3)
    score_span = 2 ** 20
    hot_dev = jax.random.randint(key_hot, (DEVICES,), 0, EXPERTS)
    hot_tok = jnp.repeat(hot_dev, TOKENS)
    forced = (jnp.arange(ROWS) % TOKENS) < CAPACITY
    outer_ids = jnp.arange(OUTER)
    grp_score = jax.random.randint(key_grp, (ROWS, OUTER), 0, score_span) * OUTER + outer_ids[None, :]
    grp_boost = forced[:, None] & (outer_ids[None, :] == (hot_tok // PER_OUTER)[:, None])
    grp_score = jnp.where(grp_boost, score_span * OUTER, grp_score)
    groups = jnp.argsort(-grp_score, axis=1)[:, :LIMIT]
    cand_count = LIMIT * PER_OUTER
    cand_ids = (groups[:, :, None] * PER_OUTER + jnp.arange(PER_OUTER)[None, None, :]).reshape(ROWS, cand_count)
    cand_score = jax.random.randint(key_exp, (ROWS, cand_count), 0, score_span) * cand_count + jnp.arange(cand_count)[None, :]
    cand_boost = forced[:, None] & (cand_ids == hot_tok[:, None])
    cand_score = jnp.where(cand_boost, score_span * cand_count, cand_score)
    pick_order = jnp.argsort(-cand_score, axis=1)[:, :TOPK]
    return jnp.take_along_axis(cand_ids, pick_order, axis=1).astype(jnp.int32)


def setup_inputs(seed: int = 0, part: int = 0) -> dict:
    base_key = jax.random.key(seed)
    part_key = jax.random.fold_in(base_key, part)
    key_tok, key_route = jax.random.split(part_key)
    key_router, key_gate, key_up, key_down = jax.random.split(base_key, 4)
    tokens = jax.random.normal(key_tok, (ROWS, D), jnp.float32).astype(jnp.bfloat16)
    w_router = (jax.random.normal(key_router, (D, EXPERTS), jnp.float32) * (2.0 / D ** 0.5)).astype(jnp.bfloat16)
    routes = draw_routes(key_route)
    w_gate = (jax.random.normal(key_gate, (EXPERTS, D, FF), jnp.float32) * D ** -0.5).astype(jnp.bfloat16)
    w_up = (jax.random.normal(key_up, (EXPERTS, D, FF), jnp.float32) * D ** -0.5).astype(jnp.bfloat16)
    w_down = (jax.random.normal(key_down, (EXPERTS, FF, D), jnp.float32) * FF ** -0.5).astype(jnp.bfloat16)
    return {'tokens': tokens, 'w_router': w_router, 'routes': routes, 'w_gate': w_gate, 'w_up': w_up, 'w_down': w_down}


def reference(tokens, w_router, routes, w_gate, w_up, w_down):
    logits = jnp.dot(tokens, w_router, preferred_element_type=jnp.float32)
    gate_vals = jax.nn.softmax(jnp.take_along_axis(logits, routes, axis=1), axis=-1)
    flat_ids = routes.reshape(DEVICES, TOKENS * TOPK)
    onehot = (flat_ids[:, :, None] == jnp.arange(EXPERTS)[None, None, :]).astype(jnp.int32)
    slot_pos = jnp.sum((jnp.cumsum(onehot, axis=1) - onehot) * onehot, axis=2)
    src_ids = jnp.arange(DEVICES)[:, None]
    total_slots = EXPERTS * DEVICES * CAPACITY
    dest_slot = jnp.where(slot_pos < CAPACITY, flat_ids * (DEVICES * CAPACITY) + src_ids * CAPACITY + slot_pos, total_slots).reshape(-1)
    pair_tok = jnp.arange(ROWS * TOPK, dtype=jnp.int32) // TOPK
    slot_tok = jnp.full((total_slots,), ROWS, jnp.int32).at[dest_slot].set(pair_tok, mode='drop')
    slot_gate = jnp.zeros((total_slots,), jnp.float32).at[dest_slot].set(gate_vals.reshape(-1), mode='drop')

    def expert_step(accum, operands):
        rows_tok, rows_gate, gate_mat, up_mat, down_mat = operands
        picked = jnp.take(tokens, rows_tok, axis=0, mode='fill', fill_value=0)
        gate_act = jnp.dot(picked, gate_mat, preferred_element_type=jnp.float32)
        up_lin = jnp.dot(picked, up_mat, preferred_element_type=jnp.float32)
        hidden = (jax.nn.silu(gate_act) * up_lin).astype(jnp.bfloat16)
        expert_out = jnp.dot(hidden, down_mat, preferred_element_type=jnp.float32).astype(jnp.bfloat16)
        accum = accum.at[rows_tok].add(rows_gate[:, None] * expert_out.astype(jnp.float32), mode='drop')
        return accum, None

    accum_init = jnp.zeros((ROWS, D), jnp.float32)
    operands = (slot_tok.reshape(EXPERTS, DEVICES * CAPACITY), slot_gate.reshape(EXPERTS, DEVICES * CAPACITY), w_gate, w_up, w_down)
    combined, _ = lax.scan(expert_step, accum_init, operands)
    return combined.astype(jnp.bfloat16)
```

```python
import jax
import jax.numpy as jnp
from jax import lax
from jax.experimental import pallas as pl
from jax.experimental.pallas import tpu as pltpu
from jax.sharding import PartitionSpec as P

MESH = pl.DeviceIdType.MESH
BF16 = jnp.bfloat16
F32 = jnp.float32
LANES = 128


def local_routes(tokens, w_router, routes, num_dev, capacity):
    tok_count, top_k = routes.shape
    num_exp = w_router.shape[1]
    per_dev = num_exp // num_dev
    logits = jnp.dot(tokens, w_router, preferred_element_type=jnp.float32)
    gate_vals = jax.nn.softmax(jnp.take_along_axis(logits, routes, axis=1), axis=-1)
    flat_ids = routes.reshape(-1)
    onehot = (flat_ids[:, None] == jnp.arange(num_exp)[None, :]).astype(jnp.int32)
    slot_pos = jnp.sum((jnp.cumsum(onehot, axis=0) - onehot) * onehot, axis=1)
    total_slots = num_exp * capacity
    send_pos = (flat_ids % per_dev) * (num_dev * capacity) + (flat_ids // per_dev) * capacity + slot_pos
    dest_slot = jnp.where(slot_pos < capacity, send_pos, total_slots)
    pair_tok = jnp.arange(tok_count * top_k, dtype=jnp.int32) // top_k
    slot_tok = jnp.full((total_slots,), tok_count, jnp.int32).at[dest_slot].set(pair_tok, mode='drop')
    return gate_vals, dest_slot, slot_tok


def expert_ffn(expert_in, w_gate, w_up, w_down):
    gate_act = jnp.einsum('erd,edf->erf', expert_in, w_gate, preferred_element_type=jnp.float32)
    up_lin = jnp.einsum('erd,edf->erf', expert_in, w_up, preferred_element_type=jnp.float32)
    hidden = (jax.nn.silu(gate_act) * up_lin).astype(jnp.bfloat16)
    return jnp.einsum('erf,efd->erd', hidden, w_down, preferred_element_type=jnp.float32).astype(jnp.bfloat16)


def plain_layer(tokens, w_router, routes, w_gate, w_up, w_down, outer_size, group_size, capacity):
    num_dev = outer_size * group_size
    tok_count, top_k = routes.shape
    model_dim = tokens.shape[1]
    num_exp = w_router.shape[1]
    per_dev = w_gate.shape[0]
    gate_vals, dest_slot, slot_tok = local_routes(tokens, w_router, routes, num_dev, capacity)
    send_buf = jnp.take(tokens, slot_tok, axis=0, mode='fill', fill_value=0)
    send_buf = send_buf.reshape(per_dev, outer_size, group_size, capacity, model_dim)
    recv_buf = lax.all_to_all(send_buf, 'outer', 1, 1, tiled=True)
    recv_buf = lax.all_to_all(recv_buf, 'expert', 2, 2, tiled=True)
    expert_out = expert_ffn(recv_buf.reshape(per_dev, num_dev * capacity, model_dim), w_gate, w_up, w_down)
    back_buf = expert_out.reshape(per_dev, outer_size, group_size, capacity, model_dim)
    back_buf = lax.all_to_all(back_buf, 'expert', 2, 2, tiled=True)
    back_buf = lax.all_to_all(back_buf, 'outer', 1, 1, tiled=True)
    picked = jnp.take(back_buf.reshape(num_exp * capacity, model_dim), dest_slot, axis=0, mode='fill', fill_value=0)
    weighted = gate_vals[:, :, None] * picked.reshape(tok_count, top_k, model_dim).astype(jnp.float32)
    return jnp.sum(weighted, axis=1).astype(jnp.bfloat16)


ROWS_CAP = 192
CHUNKS = 4
NBLK = 512
GATE_ROWS = 40
META_ROWS = 88


def moe_kernel(capacity, tok_hbm, routes_ref, wr_ref, wg_hbm, wu_hbm, wd_hbm, out_ref, flag_ref,
               X, M, Wg, Wu, Wd, Xs, Ob, Pt, Rd, Rx, TL, TS, TR, Lg, Kc,
               tok_send, tok_recv, meta_send, meta_recv, d_send, d_recv, x_send, x_recv, y_send, y_recv, w_sem, loc_sem):
    data = lax.axis_index('data')
    o = lax.axis_index('outer')
    e = lax.axis_index('expert')
    x = e // 2
    c = e % 2
    me = o * 4 + e
    num_tok, dim = tok_hbm.shape
    num_exp = wr_ref.shape[1]
    per_dev = wg_hbm.shape[0]
    cap = ROWS_CAP
    ck_rows = cap // CHUNKS
    id_p = (data, o, x * 2 + 1 - c)
    id_x = (data, o, (1 - x) * 2 + c)
    id_y = (data, 1 - o, e)

    def home(dy, dx, hc):
        return lax.rem(o + dy, 2) * 4 + lax.rem(x + dx, 2) * 2 + hc

    h_x, h_y, h_d = home(0, 1, c), home(1, 0, c), home(1, 1, c)

    barrier = pltpu.get_barrier_semaphore()
    for dev in (id_p, id_x, id_y):
        pl.semaphore_signal(barrier, inc=1, device_id=dev, device_id_type=MESH)
    pl.semaphore_wait(barrier, 3)

    def tok_copy(slot, h, dev, own=False):
        return pltpu.make_async_remote_copy(
            src_ref=tok_hbm if own else X.at[h], dst_ref=X.at[h], send_sem=tok_send.at[slot],
            recv_sem=tok_recv.at[h], device_id=dev, device_id_type=MESH)

    def meta_copy(slot, h, dev):
        return pltpu.make_async_remote_copy(
            src_ref=M.at[h], dst_ref=M.at[h], send_sem=meta_send.at[slot],
            recv_sem=meta_recv.at[h], device_id=dev, device_id_type=MESH)

    load_tok = pltpu.make_async_copy(tok_hbm, X.at[me], loc_sem.at[0])
    load_tok.start()
    sends = [(0, me, id_x), (1, me, id_y), (2, me, id_p), (3, h_x, id_y), (4, h_x, id_p), (5, h_y, id_p), (6, h_d, id_p)]
    for slot, h, dev in sends[:3]:
        tok_copy(slot, h, dev, own=True).start()

    def weight_copies(j):
        return [pltpu.make_async_copy(src.at[j], dst.at[j], w_sem.at[k, j])
                for k, (src, dst) in enumerate(((wg_hbm, Wg), (wu_hbm, Wu), (wd_hbm, Wd)))]

    for j in range(per_dev):
        for cp in weight_copies(j):
            cp.start()

    load_tok.wait()
    Lg[...] = jnp.zeros_like(Lg)
    Lg[:, 0:num_exp] = jnp.dot(X[me], wr_ref[...], preferred_element_type=F32)
    logits = Lg[...]
    lane = lax.broadcasted_iota(jnp.int32, (num_tok, LANES), 1)
    routes = routes_ref[...]
    routed = lane == routes[:, 0:1]
    for j in range(1, routes.shape[1]):
        routed = jnp.logical_or(routed, lane == routes[:, j:j + 1])
    top = jnp.max(jnp.where(routed, logits, -jnp.inf), axis=1, keepdims=True)
    ex = jnp.where(routed, jnp.exp(jnp.where(routed, logits - top, 0.0)), 0.0)
    gates = ex / jnp.sum(ex, axis=1, keepdims=True)
    routed_f = jnp.where(routed, 1.0, 0.0)
    upper = jnp.max(jnp.where(lane >= num_exp // 2, routed_f, 0.0), axis=1, keepdims=True)
    marks = routed_f + jnp.where(lane == num_exp, 1.0 - upper, 0.0) + jnp.where(lane == num_exp + 1, upper, 0.0)
    earlier = (lax.broadcasted_iota(jnp.int32, (num_tok, num_tok), 1) < lax.broadcasted_iota(jnp.int32, (num_tok, num_tok), 0))
    before = jnp.dot(jnp.where(earlier, 1.0, 0.0).astype(BF16), marks.astype(BF16), preferred_element_type=F32)
    kept = jnp.logical_and(marks > 0.5, jnp.logical_or(lane >= num_exp, before < capacity))
    rank = jnp.where(kept, before, -1.0)
    n_up = jnp.sum(upper, axis=0, keepdims=True)
    over = jnp.where(jnp.maximum(n_up, num_tok - n_up) > cap, 1.0, 0.0)
    rank = jnp.where(lane == num_exp + 2, over, rank)
    Kc[...] = rank
    gates = jnp.where(kept, gates, 0.0)
    M[me, 0:GATE_ROWS, :] = jnp.transpose(gates)[0:GATE_ROWS]
    M[me, GATE_ROWS:META_ROWS, :] = jnp.transpose(rank)[0:META_ROWS - GATE_ROWS]
    for slot, h, dev in sends[:3]:
        meta_copy(slot, h, dev).start()

    slot_iota = lax.broadcasted_iota(jnp.int32, (capacity, num_tok), 0).astype(F32)
    rank_iota = lax.broadcasted_iota(jnp.int32, (cap, num_tok), 0).astype(F32)

    def fill(h, hc):
        parts = []
        for j in range(per_dev):
            pos = M[h, pl.ds(GATE_ROWS + me * per_dev + j, 1), :]
            parts.append(jnp.where(pos == slot_iota, 1.0, 0.0).astype(BF16))
        pick = jnp.concatenate(parts, axis=0)
        for n in range(0, dim, NBLK):
            rows = jnp.dot(pick, X[h, :, n:n + NBLK], preferred_element_type=F32).astype(BF16)
            for j in range(per_dev):
                Xs[j, hc * capacity:(hc + 1) * capacity, n:n + NBLK] = rows[j * capacity:(j + 1) * capacity]

    def combine(h, hc):
        parts = []
        for j in range(per_dev):
            pos = M[h, pl.ds(GATE_ROWS + me * per_dev + j, 1), :]
            gate = M[h, pl.ds(me * per_dev + j, 1), :]
            parts.append(jnp.where(pos == slot_iota, gate, 0.0))
        spread = jnp.concatenate(parts, axis=0)
        where_to = jnp.where(M[h, pl.ds(GATE_ROWS + num_exp + o, 1), :] == rank_iota, 1.0, 0.0).astype(BF16)
        weights = []
        for _ in range(3):
            part = spread.astype(BF16)
            spread = spread - part.astype(F32)
            weights.append(lax.dot_general(where_to, part, (((1,), (1,)), ((), ())), preferred_element_type=F32).astype(BF16))
        for n in range(0, dim, NBLK):
            outs = Ob[hc, :, n:n + NBLK]
            acc = jnp.dot(weights[0], outs, preferred_element_type=F32)
            acc += jnp.dot(weights[1], outs, preferred_element_type=F32)
            acc += jnp.dot(weights[2], outs, preferred_element_type=F32)
            Pt[h, :, n:n + NBLK] = acc

    def d_copy(chip):
        return pltpu.make_async_remote_copy(
            src_ref=Pt.at[chip * 2 + 1 - c], dst_ref=Rd.at[chip], send_sem=d_send.at[chip], recv_sem=d_recv.at[chip],
            device_id=id_p, device_id_type=MESH)

    def x_copy(chip, ho, k):
        rows = pl.ds(k * ck_rows, ck_rows)
        return pltpu.make_async_remote_copy(
            src_ref=Pt.at[chip * 2 + c, rows], dst_ref=Rx.at[ho, rows], send_sem=x_send.at[ho, k], recv_sem=x_recv.at[ho, k],
            device_id=id_x, device_id_type=MESH)

    def y_copy(k):
        rows = pl.ds(k * ck_rows, ck_rows)
        return pltpu.make_async_remote_copy(
            src_ref=TS.at[rows], dst_ref=TR.at[rows], send_sem=y_send.at[k], recv_sem=y_recv.at[k],
            device_id=id_y, device_id_type=MESH)

    def arrived(h):
        tok_copy(0, h, id_p).wait_recv()
        meta_copy(0, h, id_p).wait_recv()

    def forward(which):
        slot, h, dev = sends[which]
        tok_copy(slot, h, dev).start()
        meta_copy(slot, h, dev).start()

    def group(g, carry):
        hx, ho = lax.rem(x + lax.rem(g, 2), 2), lax.rem(o + g // 2, 2)
        chip = ho * 2 + hx

        @pl.when(g == 1)
        def _():
            arrived(h_x)
            forward(3)
            forward(4)
            arrived(h_y)
            forward(5)

        @pl.when(g == 3)
        def _():
            arrived(h_d)
            forward(6)

        arrived(chip * 2 + 1 - c)
        for hc in range(2):
            fill(chip * 2 + hc, hc)

        def expert(j, carry):
            @pl.when(g == 0)
            def _():
                for cp in weight_copies(j):
                    cp.wait()

            rows = Xs[j]
            act = jnp.dot(rows, Wg[j], preferred_element_type=F32)
            lin = jnp.dot(rows, Wu[j], preferred_element_type=F32)
            hidden = (jax.nn.silu(act) * lin).astype(BF16)
            for n in range(0, dim, NBLK):
                res = jnp.dot(hidden, Wd[j, :, n:n + NBLK], preferred_element_type=F32).astype(BF16)
                for hc in range(2):
                    Ob[hc, pl.ds(pl.multiple_of(j * capacity, capacity), capacity), n:n + NBLK] = res[hc * capacity:(hc + 1) * capacity]
            return carry

        lax.fori_loop(0, per_dev, expert, 0)
        for hc in range(2):
            combine(chip * 2 + hc, hc)
        d_copy(chip).start()
        d_copy(chip).wait_recv()
        for k in range(CHUNKS):
            rows = pl.ds(k * ck_rows, ck_rows)
            Pt[chip * 2 + c, rows, :] = Pt[chip * 2 + c, rows, :] + Rd[chip, rows, :]

            @pl.when(lax.rem(g, 2) == 1)
            def _():
                x_copy(chip, ho, k).start()
        return carry

    lax.fori_loop(0, 4, group, 0)

    own = me
    for k in range(CHUNKS):
        rows = pl.ds(k * ck_rows, ck_rows)
        x_copy(0, o, k).wait_recv()
        TL[rows, :] = (Pt[own, rows, :] + Rx[o, rows, :]).astype(BF16)
    for k in range(CHUNKS):
        rows = pl.ds(k * ck_rows, ck_rows)
        x_copy(0, 1 - o, k).wait_recv()
        TS[rows, :] = (Pt[h_y, rows, :] + Rx[1 - o, rows, :]).astype(BF16)
        y_copy(k).start()

    over_all = M[0, GATE_ROWS + num_exp + 2:GATE_ROWS + num_exp + 3, :]
    for h in range(1, 8):
        over_all = jnp.maximum(over_all, M[h, GATE_ROWS + num_exp + 2:GATE_ROWS + num_exp + 3, :])
    flag_ref[...] = jnp.broadcast_to(jnp.max(over_all, axis=1, keepdims=True), flag_ref.shape)

    cap_iota = lax.broadcasted_iota(jnp.int32, (num_tok, cap), 1).astype(F32)
    rank_0, rank_1 = Kc[:, num_exp:num_exp + 1], Kc[:, num_exp + 1:num_exp + 2]
    here = jnp.where(o == 0, rank_0, rank_1)
    there = jnp.where(o == 0, rank_1, rank_0)
    take_here = jnp.where(here == cap_iota, 1.0, 0.0).astype(BF16)
    take_there = jnp.where(there == cap_iota, 1.0, 0.0).astype(BF16)
    for k in range(CHUNKS):
        y_copy(k).wait_recv()
    for n in range(0, dim, NBLK):
        acc = jnp.dot(take_here, TL[:, n:n + NBLK], preferred_element_type=F32)
        acc += jnp.dot(take_there, TR[:, n:n + NBLK], preferred_element_type=F32)
        out_ref[:, n:n + NBLK] = acc.astype(BF16)

    for slot, h, dev in sends:
        tok_copy(slot, h, dev).wait_send()
        meta_copy(slot, h, dev).wait_send()
    for chip in range(4):
        d_copy(chip).wait_send()
    for k in range(CHUNKS):
        for ho in range(2):
            x_copy(0, ho, k).wait_send()
        y_copy(k).wait_send()


def solution(mesh):
    outer_size = mesh.shape['outer']
    group_size = mesh.shape['expert']
    row_spec = P(('data', 'outer', 'expert'), None)
    weight_spec = P(('outer', 'expert'), None, None)

    def per_device(tokens, w_router, routes, w_gate, w_up, w_down):
        tok_count, top_k = routes.shape
        dim = tokens.shape[1]
        num_exp = w_router.shape[1]
        per_dev, _, ffn = w_gate.shape
        capacity = (5 * tok_count * top_k + 4 * num_exp - 1) // (4 * num_exp)
        homes = outer_size * group_size
        cap = ROWS_CAP
        vmem = pl.BlockSpec(memory_space=pltpu.VMEM)
        hbm = pl.BlockSpec(memory_space=pl.ANY)
        dma = pltpu.SemaphoreType.DMA

        def body(*refs):
            moe_kernel(capacity, *refs)

        fast, flag = pl.pallas_call(
            body,
            out_shape=(jax.ShapeDtypeStruct((tok_count, dim), BF16), jax.ShapeDtypeStruct((8, LANES), F32)),
            in_specs=[hbm, vmem, vmem, hbm, hbm, hbm],
            out_specs=(vmem, vmem),
            scratch_shapes=[
                pltpu.VMEM((homes, tok_count, dim), BF16),
                pltpu.VMEM((homes, META_ROWS, tok_count), F32),
                pltpu.VMEM((per_dev, dim, ffn), BF16),
                pltpu.VMEM((per_dev, dim, ffn), BF16),
                pltpu.VMEM((per_dev, ffn, dim), BF16),
                pltpu.VMEM((per_dev, 2 * capacity, dim), BF16),
                pltpu.VMEM((2, per_dev * capacity, dim), BF16),
                pltpu.VMEM((homes, cap, dim), F32),
                pltpu.VMEM((homes // 2, cap, dim), F32),
                pltpu.VMEM((2, cap, dim), F32),
                pltpu.VMEM((cap, dim), BF16),
                pltpu.VMEM((cap, dim), BF16),
                pltpu.VMEM((cap, dim), BF16),
                pltpu.VMEM((tok_count, LANES), F32),
                pltpu.VMEM((tok_count, LANES), F32),
                dma((7,)), dma((homes,)), dma((7,)), dma((homes,)),
                dma((4,)), dma((4,)),
                dma((2, CHUNKS)), dma((2, CHUNKS)), dma((CHUNKS,)), dma((CHUNKS,)),
                dma((3, per_dev)), dma((1,)),
            ],
            compiler_params=pltpu.CompilerParams(collective_id=0, has_side_effects=True, vmem_limit_bytes=66_000_000),
            name='moe',
        )(tokens, routes, w_router, w_gate, w_up, w_down)

        def slow():
            return plain_layer(tokens, w_router, routes, w_gate, w_up, w_down, outer_size, group_size, capacity)

        return lax.cond(flag[0, 0] > 0.5, slow, lambda: fast)

    return jax.shard_map(per_device, mesh=mesh, in_specs=(row_spec, P(), row_spec, weight_spec, weight_spec, weight_spec), out_specs=row_spec, check_vma=False)
```

```python
import jax
import jax.numpy as jnp
from jax import lax
from jax.experimental import pallas as pl
from jax.experimental.pallas import tpu as pltpu
from jax.sharding import PartitionSpec as P

MESH = pl.DeviceIdType.MESH
BF16 = jnp.bfloat16
F32 = jnp.float32
LANES = 128


def local_routes(tokens, w_router, routes, num_dev, capacity):
    tok_count, top_k = routes.shape
    num_exp = w_router.shape[1]
    per_dev = num_exp // num_dev
    logits = jnp.dot(tokens, w_router, preferred_element_type=jnp.float32)
    gate_vals = jax.nn.softmax(jnp.take_along_axis(logits, routes, axis=1), axis=-1)
    flat_ids = routes.reshape(-1)
    onehot = (flat_ids[:, None] == jnp.arange(num_exp)[None, :]).astype(jnp.int32)
    slot_pos = jnp.sum((jnp.cumsum(onehot, axis=0) - onehot) * onehot, axis=1)
    total_slots = num_exp * capacity
    send_pos = (flat_ids % per_dev) * (num_dev * capacity) + (flat_ids // per_dev) * capacity + slot_pos
    dest_slot = jnp.where(slot_pos < capacity, send_pos, total_slots)
    pair_tok = jnp.arange(tok_count * top_k, dtype=jnp.int32) // top_k
    slot_tok = jnp.full((total_slots,), tok_count, jnp.int32).at[dest_slot].set(pair_tok, mode='drop')
    return gate_vals, dest_slot, slot_tok


def expert_ffn(expert_in, w_gate, w_up, w_down):
    gate_act = jnp.einsum('erd,edf->erf', expert_in, w_gate, preferred_element_type=jnp.float32)
    up_lin = jnp.einsum('erd,edf->erf', expert_in, w_up, preferred_element_type=jnp.float32)
    hidden = (jax.nn.silu(gate_act) * up_lin).astype(jnp.bfloat16)
    return jnp.einsum('erf,efd->erd', hidden, w_down, preferred_element_type=jnp.float32).astype(jnp.bfloat16)


def plain_layer(tokens, w_router, routes, w_gate, w_up, w_down, outer_size, group_size, capacity):
    num_dev = outer_size * group_size
    tok_count, top_k = routes.shape
    model_dim = tokens.shape[1]
    num_exp = w_router.shape[1]
    per_dev = w_gate.shape[0]
    gate_vals, dest_slot, slot_tok = local_routes(tokens, w_router, routes, num_dev, capacity)
    send_buf = jnp.take(tokens, slot_tok, axis=0, mode='fill', fill_value=0)
    send_buf = send_buf.reshape(per_dev, outer_size, group_size, capacity, model_dim)
    recv_buf = lax.all_to_all(send_buf, 'outer', 1, 1, tiled=True)
    recv_buf = lax.all_to_all(recv_buf, 'expert', 2, 2, tiled=True)
    expert_out = expert_ffn(recv_buf.reshape(per_dev, num_dev * capacity, model_dim), w_gate, w_up, w_down)
    back_buf = expert_out.reshape(per_dev, outer_size, group_size, capacity, model_dim)
    back_buf = lax.all_to_all(back_buf, 'expert', 2, 2, tiled=True)
    back_buf = lax.all_to_all(back_buf, 'outer', 1, 1, tiled=True)
    picked = jnp.take(back_buf.reshape(num_exp * capacity, model_dim), dest_slot, axis=0, mode='fill', fill_value=0)
    weighted = gate_vals[:, :, None] * picked.reshape(tok_count, top_k, model_dim).astype(jnp.float32)
    return jnp.sum(weighted, axis=1).astype(jnp.bfloat16)


ROWS_CAP = 184
Y_ROWS = 192
NBLK = 256
UNROUTED, DROPPED = -1.0, -2.0

ORDER = ((0, 0, 0), (0, 0, 1), (0, 1, 0), (1, 0, 1), (0, 1, 1), (1, 0, 0), (1, 1, 0), (1, 1, 1))
DY_BITS, DX_BITS, HC_BITS = (sum(place[i] << n for n, place in enumerate(ORDER)) for i in range(3))
TILE = 256


def bit(table, i):
    return lax.rem(lax.shift_right_logical(jnp.int32(table), i), 2)


def moe_kernel(capacity, tok_hbm, routes_hbm, wr_hbm, wg_hbm, wu_hbm, wd_hbm, out_hbm, flag_ref,
               X, M, Yo, Yf, Rt, Wr, Wg, Wu, Wd, Xs, Ob, Pt, Rd, Rx, TL, TS, TR, Ot, Over, Pg, Ps,
               tok_send, tok_recv, meta_send, meta_recv, d_send, d_recv, x_send, x_recv, y_send, y_recv, w_sem, loc_sem, out_sem):
    data = lax.axis_index('data')
    o = lax.axis_index('outer')
    e = lax.axis_index('expert')
    x = e // 2
    c = lax.rem(e, 2)
    me = o * 4 + e
    num_tok, dim = tok_hbm.shape
    num_exp = wr_hbm.shape[0]
    per_dev = wg_hbm.shape[0]
    cap = ROWS_CAP
    blocks = dim // NBLK
    half = num_exp // 2
    id_p = (data, o, x * 2 + 1 - c)
    id_x = (data, o, (1 - x) * 2 + c)
    id_y = (data, 1 - o, e)

    def home(dy, dx, hc):
        return lax.rem(o + dy, 2) * 4 + lax.rem(x + dx, 2) * 2 + hc

    h_x, h_y, h_d = home(0, 1, c), home(1, 0, c), home(1, 1, c)

    barrier = pltpu.get_barrier_semaphore()
    for dev in (id_p, id_x, id_y):
        pl.semaphore_signal(barrier, inc=1, device_id=dev, device_id_type=MESH)

    loads = [pltpu.make_async_copy(src, dst, loc_sem.at[n])
             for n, (src, dst) in enumerate(((tok_hbm, X.at[me]), (routes_hbm, Rt), (wr_hbm, Wr)))]
    for cp in loads:
        cp.start()

    def weight_copies(j):
        return [pltpu.make_async_copy(src.at[j], dst.at[j], w_sem.at[k, j])
                for k, (src, dst) in enumerate(((wg_hbm, Wg), (wu_hbm, Wu), (wd_hbm, Wd)))]

    with jax.named_scope('barrier'):
        pl.semaphore_wait(barrier, 3)

    def tok_copy(slot, h, dev, own=False):
        return pltpu.make_async_remote_copy(
            src_ref=tok_hbm if own else X.at[h], dst_ref=X.at[h], send_sem=tok_send.at[slot],
            recv_sem=tok_recv.at[h], device_id=dev, device_id_type=MESH)

    def row_copy(slot, h, src):
        return pltpu.make_async_remote_copy(
            src_ref=src, dst_ref=X.at[h, 0:Y_ROWS], send_sem=tok_send.at[slot],
            recv_sem=tok_recv.at[h], device_id=id_y, device_id_type=MESH)

    def meta_copy(slot, h, dev):
        return pltpu.make_async_remote_copy(
            src_ref=M.at[h], dst_ref=M.at[h], send_sem=meta_send.at[slot],
            recv_sem=meta_recv.at[h], device_id=dev, device_id_type=MESH)

    @pl.when(c == 0)
    def _():
        tok_copy(0, me, id_x, own=True).start()

    tok_copy(2, me, id_p, own=True).start()
    for dx in range(2):
        for hc in range(2):
            X[home(1, dx, hc), Y_ROWS:, :] = jnp.zeros((num_tok - Y_ROWS, dim), BF16)

    earlier = (lax.broadcasted_iota(jnp.int32, (num_tok, num_tok), 0) < lax.broadcasted_iota(jnp.int32, (num_tok, num_tok), 1))
    earlier = jnp.where(earlier, 1.0, 0.0).astype(BF16)

    with jax.named_scope('load_wait'):
        for cp in loads:
            cp.wait()
        for j in range(per_dev):
            for cp in weight_copies(j):
                cp.start()
    with jax.named_scope('meta'):
        logits = lax.dot_general(Wr[...], X[me], (((1,), (1,)), ((), ())), preferred_element_type=F32)
        expert_id = lax.broadcasted_iota(jnp.int32, (num_exp, num_tok), 0)
        routed = expert_id == Rt[0:1, :]
        for j in range(1, Rt.shape[0]):
            routed = jnp.logical_or(routed, expert_id == Rt[j:j + 1, :])
        top = jnp.max(jnp.where(routed, logits, -jnp.inf), axis=0, keepdims=True)
        ex = jnp.where(routed, jnp.exp(jnp.where(routed, logits - top, 0.0)), 0.0)
        gates = ex / jnp.sum(ex, axis=0, keepdims=True)
        pos = jnp.dot(jnp.where(routed, 1.0, 0.0).astype(BF16), earlier, preferred_element_type=F32)
        M[me] = jnp.where(routed, jnp.where(pos < capacity, gates, DROPPED), UNROUTED)
    meta_copy(2, me, id_p).start()

    slot_iota = lax.broadcasted_iota(jnp.int32, (capacity, num_tok), 0).astype(F32)
    rank_iota = lax.broadcasted_iota(jnp.int32, (cap, num_tok), 0).astype(F32)
    row_id = lax.broadcasted_iota(jnp.int32, (num_exp, num_tok), 0)
    in_row = jnp.logical_and(row_id >= o * half, row_id < o * half + half)

    row_iota = lax.broadcasted_iota(jnp.int32, (num_tok, num_tok), 0).astype(F32)

    def row_members(h):
        hit = jnp.logical_and(M[h] != UNROUTED, in_row)
        return jnp.max(jnp.where(hit, 1.0, 0.0), axis=0, keepdims=True)

    def plan(h):
        gates = [M[h, pl.ds(me * per_dev + j, 1), :] for j in range(per_dev)]
        members = row_members(h)
        marks = [jnp.where(g != UNROUTED, 1.0, 0.0) for g in gates] + [members]
        marks += [jnp.zeros_like(members)] * (8 - len(marks))
        before = jnp.dot(jnp.concatenate(marks, axis=0).astype(BF16), earlier, preferred_element_type=F32)
        slots = [jnp.where(g >= 0.0, before[j:j + 1], -1.0) for j, g in enumerate(gates)]
        rank = jnp.where(members > 0.5, before[per_dev:per_dev + 1], -1.0)
        return gates, slots, rank, members

    def compact(h, dst):
        others = 1.0 - row_members(h)
        before = jnp.dot(jnp.concatenate([others] * 8, axis=0).astype(BF16), earlier, preferred_element_type=F32)
        rank = jnp.where(others > 0.5, before[0:1], -1.0)
        sel = jnp.where(rank == row_iota[0:Y_ROWS], 1.0, 0.0).astype(BF16)
        dst[...] = jnp.dot(sel, X[h], preferred_element_type=F32).astype(BF16)

    with jax.named_scope('compact'):
        compact(me, Yo)

    @pl.when(c == 0)
    def _():
        meta_copy(0, me, id_x).start()

    @pl.when(c == 1)
    def _():
        meta_copy(0, me, id_y).start()
        row_copy(0, me, Yo).start()

    def d_copy(chip, k):
        return pltpu.make_async_remote_copy(
            src_ref=Pt.at[chip * 2 + 1 - c, k], dst_ref=Rd.at[chip, k], send_sem=d_send.at[chip, k],
            recv_sem=d_recv.at[chip, k], device_id=id_p, device_id_type=MESH)

    def x_copy(ho, k):
        return pltpu.make_async_remote_copy(
            src_ref=Pt.at[ho * 4 + (1 - x) * 2 + c, k], dst_ref=Rx.at[ho, k], send_sem=x_send.at[ho, k],
            recv_sem=x_recv.at[ho, k], device_id=id_x, device_id_type=MESH)

    def y_copy(k):
        return pltpu.make_async_remote_copy(
            src_ref=TS.at[k], dst_ref=TR.at[k], send_sem=y_send.at[k], recv_sem=y_recv.at[k],
            device_id=id_y, device_id_type=MESH)

    def out_copy(k):
        return pltpu.make_async_copy(Ot.at[:, k * NBLK:(k + 1) * NBLK], out_hbm.at[:, k * NBLK:(k + 1) * NBLK], out_sem.at[k])

    def arrived(h, rows=False):
        if rows:
            row_copy(0, h, Yo).wait_recv()
        else:
            tok_copy(0, h, id_p).wait_recv()
        meta_copy(0, h, id_p).wait_recv()

    def rows_to_partner(slot, h):
        return pltpu.make_async_remote_copy(
            src_ref=X.at[h, 0:Y_ROWS], dst_ref=X.at[h, 0:Y_ROWS], send_sem=tok_send.at[slot],
            recv_sem=tok_recv.at[h], device_id=id_p, device_id_type=MESH)

    def to_partner(slot, h, rows=False):
        if rows:
            rows_to_partner(slot, h).start()
        else:
            tok_copy(slot, h, id_p).start()
        meta_copy(slot, h, id_p).start()

    def at(cond, name, body):
        @pl.when(cond)
        def _():
            with jax.named_scope(name):
                body()

    def own_along_y():
        meta_copy(1, me, id_y).start()
        row_copy(1, me, Yo).start()

    def own_along_x():
        meta_copy(1, me, id_x).start()
        tok_copy(1, me, id_x, own=True).start()

    def forward_x():
        compact(h_x, Yf)
        meta_copy(6, h_x, id_y).start()
        row_copy(6, h_x, Yf).start()

    def x_arrived():
        arrived(h_x)
        to_partner(3, h_x)

    def y_arrived():
        arrived(h_y, rows=True)
        to_partner(4, h_y, rows=True)

    def d_arrived():
        arrived(h_d, rows=True)
        to_partner(5, h_d, rows=True)

    def first_arrived():
        @pl.when(c == 0)
        def _():
            x_arrived()
            forward_x()

        @pl.when(c == 1)
        def _():
            y_arrived()

    def x1_arrived():
        x_arrived()
        forward_x()

    def finish(ho, last):
        chip = ho * 2 + 1 - x
        for k in range(blocks):
            d_copy(chip, k).wait_recv()
            Pt[chip * 2 + c, k] = Pt[chip * 2 + c, k] + Rd[chip, k]
            if last or k < blocks - 1:
                x_copy(ho, k).start()
        if last:
            x_copy(o, blocks - 1).start()

    Over[...] = jnp.zeros_like(Over)
    token_id = lax.broadcasted_iota(jnp.int32, (1, num_tok), 1).astype(F32)

    def place(n):
        dy, dx, hc = bit(DY_BITS, n), bit(DX_BITS, n), bit(HC_BITS, n)
        return home(dy, dx, hc), dy, hc

    def out_slot(n):
        return jnp.where(n < 2, 4 + n, lax.rem(n + 2, 4))

    def combine(i, m):
        n = lax.rem(2 * i + m, 8)
        outs = out_slot(n)
        h, dy, hc = place(n)
        with jax.named_scope('combine'):
            gates, slots = Pg[n], Ps[n]
            spread = jnp.concatenate([jnp.where(slots[j:j + 1] == slot_iota, gates[j:j + 1], 0.0) for j in range(per_dev)], axis=0)
            where_to = jnp.where(slots[per_dev:per_dev + 1] == rank_iota, 1.0, 0.0).astype(BF16)
            parts = []
            for _ in range(3):
                parts.append(spread.astype(BF16))
                spread = spread - parts[-1].astype(F32)
            tiles = [p[0:TILE] for p in parts] + [jnp.concatenate([p[TILE:] for p in parts], axis=0)]
            weights = [lax.dot_general(where_to, t, (((1,), (1,)), ((), ())), preferred_element_type=F32).astype(BF16)
                       for t in tiles]
            for k in range(blocks):
                cols = slice(k * NBLK, (k + 1) * NBLK)
                acc = jnp.dot(weights[3], Ob[outs, TILE:, cols], preferred_element_type=F32)
                for w in weights[:3]:
                    acc += jnp.dot(w, Ob[outs, 0:TILE, cols], preferred_element_type=F32)
                Pt[h, k] = acc

        @pl.when(hc != c)
        def _():
            for k in range(blocks):
                d_copy(h // 2, k).start()

    def step(i, carry):
        places = [place(2 * i), place(2 * i + 1)]
        for h, dy, hc in places:
            at(jnp.logical_and(hc != c, dy == 0), 'wait_other', lambda h=h: arrived(h))
            at(jnp.logical_and(hc != c, dy == 1), 'wait_other', lambda h=h: arrived(h, rows=True))

        with jax.named_scope('fill'):
            for n, (h, dy, hc) in enumerate(places):
                gates, slots, rank, members = plan(h)
                count = jnp.sum(members, axis=1, keepdims=True)
                Over[...] = jnp.maximum(Over[...], jnp.maximum(count, num_tok - count))
                pad = [jnp.full_like(rank, -1.0)] * (8 - per_dev - 1)
                stored = jnp.concatenate(slots + [rank] + pad, axis=0)
                Ps[2 * i + n] = stored
                Pg[2 * i + n] = jnp.concatenate(gates + [rank] + pad, axis=0)
                key = jnp.where(dy == 1, rank, token_id)
                held = lax.dot_general((stored + 1.0).astype(BF16), jnp.where(key == row_iota, 1.0, 0.0).astype(BF16),
                                       (((1,), (1,)), ((), ())), preferred_element_type=F32) - 1.0
                pick = jnp.concatenate([jnp.where(held[j:j + 1] == slot_iota, 1.0, 0.0).astype(BF16) for j in range(per_dev)], axis=0)
                for k in range(blocks):
                    cols = slice(k * NBLK, (k + 1) * NBLK)
                    rows = jnp.dot(pick, X[h, :, cols], preferred_element_type=F32).astype(BF16)
                    for j in range(per_dev):
                        Xs[j, n * capacity:(n + 1) * capacity, cols] = rows[j * capacity:(j + 1) * capacity]

        @pl.when(i == 0)
        def _():
            for j in range(per_dev):
                for cp in weight_copies(j):
                    cp.wait()

            @pl.when(c == 0)
            def _():
                own_along_y()

        with jax.named_scope('experts'):
            for j in range(per_dev):
                if j == 2:
                    at(jnp.logical_and(i == 0, c == 1), 'own_along_x', own_along_x)
                rows = Xs[j]
                act = jnp.dot(rows, Wg[j], preferred_element_type=F32)
                lin = jnp.dot(rows, Wu[j], preferred_element_type=F32)
                hidden = (jax.nn.silu(act) * lin).astype(BF16)
                res = jnp.dot(hidden, Wd[j], preferred_element_type=F32).astype(BF16)
                for n in range(2):
                    part = res[n * capacity:(n + 1) * capacity]
                    slot = out_slot(2 * i + n)
                    Ob[slot, j * capacity:(j + 1) * capacity, :] = part
                    if (j + 1) * capacity > TILE:
                        for copy in (1, 2):
                            lo = j * capacity + copy * (per_dev * capacity - TILE)
                            Ob[slot, lo:lo + capacity, :] = part

        at(i == 0, 'first_arrived', first_arrived)

        def part(m, carry):
            at(jnp.logical_and(i == 2, m == 1), 'wait_hd', d_arrived)
            at(jnp.logical_and(jnp.logical_and(i == 1, m == 1), c == 0), 'wait_hy0', y_arrived)
            combine(i, m)
            at(jnp.logical_and(jnp.logical_and(i == 1, m == 1), c == 1), 'wait_hx1', x1_arrived)
            at(jnp.logical_and(jnp.logical_and(i == 1, m == 1), c == 0), 'finish_x0', lambda: finish(o, False))
            at(jnp.logical_and(jnp.logical_and(i == 2, m == 1), c == 1), 'finish_x1', lambda: finish(o, False))
            at(jnp.logical_and(i == 3, m == 1 + c), 'finish_d', lambda: finish(1 - o, True))
            return carry

        lax.fori_loop(0, jnp.where(i == 0, 0, jnp.where(i == 3, 4, 2)), part, 0)
        return carry

    lax.fori_loop(0, 4, step, 0)
    flag_ref[0, 0] = jnp.max(Over[...])

    def total(ho, k):
        chip = ho * 2 + x
        with jax.named_scope('wait_x'):
            x_copy(ho, k).wait_recv()
        d_copy(chip, k).wait_recv()
        return (Pt[chip * 2 + c, k] + Rd[chip, k] + Rx[ho, k]).astype(BF16)

    members = row_members(me)
    marks = jnp.concatenate([members, 1.0 - members] + [jnp.zeros_like(members)] * 6, axis=0)
    before = jnp.dot(marks.astype(BF16), earlier, preferred_element_type=F32)
    ranks = jnp.where(marks > 0.5, before, -1.0)
    ranks = jnp.transpose(jnp.concatenate([ranks] * (LANES // 8), axis=0))
    cap_iota = lax.broadcasted_iota(jnp.int32, (num_tok, cap), 1).astype(F32)
    take_here = jnp.where(ranks[:, 0:1] == cap_iota, 1.0, 0.0).astype(BF16)
    take_there = jnp.where(ranks[:, 1:2] == cap_iota, 1.0, 0.0).astype(BF16)

    def emit(k):
        with jax.named_scope('wait_y'):
            y_copy(k).wait_recv()
        acc = jnp.dot(take_here, TL[k], preferred_element_type=F32)
        acc += jnp.dot(take_there, TR[k], preferred_element_type=F32)
        Ot[:, k * NBLK:(k + 1) * NBLK] = acc.astype(BF16)
        out_copy(k).start()

    for k in range(blocks - 1):
        TL[k] = total(o, k)
    for k in range(blocks):
        TS[k] = total(1 - o, k)
        y_copy(k).start()
        if k > 0:
            emit(k - 1)
    TL[blocks - 1] = total(o, blocks - 1)
    emit(blocks - 1)

    for k in range(blocks):
        out_copy(k).wait()
    @pl.when(c == 0)
    def _():
        tok_copy(0, me, id_x, own=True).wait_send()
        row_copy(1, me, Yo).wait_send()

    @pl.when(c == 1)
    def _():
        row_copy(0, me, Yo).wait_send()
        tok_copy(1, me, id_x, own=True).wait_send()

    tok_copy(2, me, id_p, own=True).wait_send()
    tok_copy(3, h_x, id_p).wait_send()
    rows_to_partner(4, h_y).wait_send()
    rows_to_partner(5, h_d).wait_send()
    row_copy(6, h_x, Yf).wait_send()
    for slot in range(7):
        meta_copy(slot, me, id_p).wait_send()
    for k in range(blocks):
        for chip in range(4):
            d_copy(chip, k).wait_send()
        for ho in range(2):
            x_copy(ho, k).wait_send()
        y_copy(k).wait_send()


def solution(mesh):
    outer_size = mesh.shape['outer']
    group_size = mesh.shape['expert']
    row_spec = P(('data', 'outer', 'expert'), None)
    weight_spec = P(('outer', 'expert'), None, None)

    def per_device(tokens, w_router, routes, w_gate, w_up, w_down):
        tok_count, top_k = routes.shape
        dim = tokens.shape[1]
        num_exp = w_router.shape[1]
        per_dev, _, ffn = w_gate.shape
        capacity = (5 * tok_count * top_k + 4 * num_exp - 1) // (4 * num_exp)
        homes = outer_size * group_size
        cap = ROWS_CAP
        blocks = dim // NBLK
        hbm = pl.BlockSpec(memory_space=pl.ANY)
        dma = pltpu.SemaphoreType.DMA

        def body(*refs):
            moe_kernel(capacity, *refs)

        fast, flag = pl.pallas_call(
            body,
            out_shape=(jax.ShapeDtypeStruct((tok_count, dim), BF16), jax.ShapeDtypeStruct((1, 1), F32)),
            in_specs=[hbm] * 6,
            out_specs=(hbm, pl.BlockSpec(memory_space=pltpu.SMEM)),
            scratch_shapes=[
                pltpu.VMEM((homes, tok_count, dim), BF16),
                pltpu.VMEM((homes, num_exp, tok_count), F32),
                pltpu.VMEM((Y_ROWS, dim), BF16),
                pltpu.VMEM((Y_ROWS, dim), BF16),
                pltpu.VMEM((top_k, tok_count), jnp.int32),
                pltpu.VMEM((num_exp, dim), BF16),
                pltpu.VMEM((per_dev, dim, ffn), BF16),
                pltpu.VMEM((per_dev, dim, ffn), BF16),
                pltpu.VMEM((per_dev, ffn, dim), BF16),
                pltpu.VMEM((per_dev, 2 * capacity, dim), BF16),
                pltpu.VMEM((6, TILE + 3 * (per_dev * capacity - TILE), dim), BF16),
                pltpu.VMEM((homes, blocks, cap, NBLK), F32),
                pltpu.VMEM((homes // 2, blocks, cap, NBLK), F32),
                pltpu.VMEM((2, blocks, cap, NBLK), F32),
                pltpu.VMEM((blocks, cap, NBLK), BF16),
                pltpu.VMEM((blocks, cap, NBLK), BF16),
                pltpu.VMEM((blocks, cap, NBLK), BF16),
                pltpu.VMEM((tok_count, dim), BF16),
                pltpu.VMEM((8, LANES), F32),
                pltpu.VMEM((homes, 8, tok_count), F32),
                pltpu.VMEM((homes, 8, tok_count), F32),
                dma((7,)), dma((homes,)), dma((7,)), dma((homes,)),
                dma((homes // 2, blocks)), dma((homes // 2, blocks)),
                dma((2, blocks)), dma((2, blocks)), dma((blocks,)), dma((blocks,)),
                dma((3, per_dev)), dma((3,)), dma((blocks,)),
            ],
            compiler_params=pltpu.CompilerParams(collective_id=0, has_side_effects=True, vmem_limit_bytes=66_000_000),
            name='moe',
        )(tokens, routes.T, w_router.T, w_gate, w_up, w_down)

        def slow():
            return plain_layer(tokens, w_router, routes, w_gate, w_up, w_down, outer_size, group_size, capacity)

        return lax.cond(flag[0, 0] > cap, slow, lambda: fast)

    return jax.shard_map(per_device, mesh=mesh, in_specs=(row_spec, P(), row_spec, weight_spec, weight_spec, weight_spec), out_specs=row_spec, check_vma=False)
```

```python
import jax
import jax.numpy as jnp
from jax import lax
from jax.experimental import pallas as pl
from jax.experimental.pallas import tpu as pltpu
from jax.sharding import PartitionSpec as P

MESH = pl.DeviceIdType.MESH
BF16 = jnp.bfloat16
F32 = jnp.float32
LANES = 128


def local_routes(tokens, w_router, routes, num_dev, capacity):
    tok_count, top_k = routes.shape
    num_exp = w_router.shape[1]
    per_dev = num_exp // num_dev
    logits = jnp.dot(tokens, w_router, preferred_element_type=jnp.float32)
    gate_vals = jax.nn.softmax(jnp.take_along_axis(logits, routes, axis=1), axis=-1)
    flat_ids = routes.reshape(-1)
    onehot = (flat_ids[:, None] == jnp.arange(num_exp)[None, :]).astype(jnp.int32)
    slot_pos = jnp.sum((jnp.cumsum(onehot, axis=0) - onehot) * onehot, axis=1)
    total_slots = num_exp * capacity
    send_pos = (flat_ids % per_dev) * (num_dev * capacity) + (flat_ids // per_dev) * capacity + slot_pos
    dest_slot = jnp.where(slot_pos < capacity, send_pos, total_slots)
    pair_tok = jnp.arange(tok_count * top_k, dtype=jnp.int32) // top_k
    slot_tok = jnp.full((total_slots,), tok_count, jnp.int32).at[dest_slot].set(pair_tok, mode='drop')
    return gate_vals, dest_slot, slot_tok


def expert_ffn(expert_in, w_gate, w_up, w_down):
    gate_act = jnp.einsum('erd,edf->erf', expert_in, w_gate, preferred_element_type=jnp.float32)
    up_lin = jnp.einsum('erd,edf->erf', expert_in, w_up, preferred_element_type=jnp.float32)
    hidden = (jax.nn.silu(gate_act) * up_lin).astype(jnp.bfloat16)
    return jnp.einsum('erf,efd->erd', hidden, w_down, preferred_element_type=jnp.float32).astype(jnp.bfloat16)


def plain_layer(tokens, w_router, routes, w_gate, w_up, w_down, outer_size, group_size, capacity):
    num_dev = outer_size * group_size
    tok_count, top_k = routes.shape
    model_dim = tokens.shape[1]
    num_exp = w_router.shape[1]
    per_dev = w_gate.shape[0]
    gate_vals, dest_slot, slot_tok = local_routes(tokens, w_router, routes, num_dev, capacity)
    send_buf = jnp.take(tokens, slot_tok, axis=0, mode='fill', fill_value=0)
    send_buf = send_buf.reshape(per_dev, outer_size, group_size, capacity, model_dim)
    recv_buf = lax.all_to_all(send_buf, 'outer', 1, 1, tiled=True)
    recv_buf = lax.all_to_all(recv_buf, 'expert', 2, 2, tiled=True)
    expert_out = expert_ffn(recv_buf.reshape(per_dev, num_dev * capacity, model_dim), w_gate, w_up, w_down)
    back_buf = expert_out.reshape(per_dev, outer_size, group_size, capacity, model_dim)
    back_buf = lax.all_to_all(back_buf, 'expert', 2, 2, tiled=True)
    back_buf = lax.all_to_all(back_buf, 'outer', 1, 1, tiled=True)
    picked = jnp.take(back_buf.reshape(num_exp * capacity, model_dim), dest_slot, axis=0, mode='fill', fill_value=0)
    weighted = gate_vals[:, :, None] * picked.reshape(tok_count, top_k, model_dim).astype(jnp.float32)
    return jnp.sum(weighted, axis=1).astype(jnp.bfloat16)


ROWS_CAP = 184
Y_ROWS = 192
NBLK = 256
UNROUTED, DROPPED = -1.0, -2.0

ORDER = ((0, 0, 0), (0, 0, 1), (0, 1, 0), (1, 0, 1), (0, 1, 1), (1, 0, 0), (1, 1, 0), (1, 1, 1))
DY_BITS, DX_BITS, HC_BITS = (sum(place[i] << n for n, place in enumerate(ORDER)) for i in range(3))
TILE = 256
SEND_AFTER = (3, 6)


def bit(table, i):
    return lax.rem(lax.shift_right_logical(jnp.int32(table), i), 2)


def moe_kernel(capacity, tok_hbm, routes_hbm, wr_hbm, wg_hbm, wu_hbm, wd_hbm, out_ref, flag_ref,
               X, M, Yo, Yf, Rt, Wr, Wg, Wu, Wd, Xs, Ob, Pt, Rd, Rx, TL, TS, TR, Over, Pg, Ps, Pick,
               tok_send, tok_recv, meta_send, meta_recv, d_send, d_recv, x_send, x_recv, y_send, y_recv, w_sem, loc_sem):
    data = lax.axis_index('data')
    o = lax.axis_index('outer')
    e = lax.axis_index('expert')
    x = e // 2
    c = lax.rem(e, 2)
    me = o * 4 + e
    num_tok, dim = tok_hbm.shape
    num_exp = wr_hbm.shape[0]
    per_dev = wg_hbm.shape[0]
    cap = ROWS_CAP
    blocks = dim // NBLK
    half = num_exp // 2
    id_p = (data, o, x * 2 + 1 - c)
    id_x = (data, o, (1 - x) * 2 + c)
    id_y = (data, 1 - o, e)

    def home(dy, dx, hc):
        return lax.rem(o + dy, 2) * 4 + lax.rem(x + dx, 2) * 2 + hc

    h_x, h_y, h_d = home(0, 1, c), home(1, 0, c), home(1, 1, c)

    barrier = pltpu.get_barrier_semaphore()
    for dev in (id_p, id_x, id_y):
        pl.semaphore_signal(barrier, inc=1, device_id=dev, device_id_type=MESH)

    loads = [pltpu.make_async_copy(src, dst, loc_sem.at[n])
             for n, (src, dst) in enumerate(((tok_hbm, X.at[me]), (routes_hbm, Rt), (wr_hbm, Wr)))]
    for cp in loads:
        cp.start()

    def weight_copies(j):
        return [pltpu.make_async_copy(src.at[j], dst.at[j], w_sem.at[k, j])
                for k, (src, dst) in enumerate(((wg_hbm, Wg), (wu_hbm, Wu), (wd_hbm, Wd)))]

    with jax.named_scope('barrier'):
        pl.semaphore_wait(barrier, 3)

    def tok_copy(slot, half, h, dev, own=False):
        rows = pl.ds(half * (num_tok // 2), num_tok // 2)
        return pltpu.make_async_remote_copy(
            src_ref=tok_hbm.at[rows] if own else X.at[h, rows], dst_ref=X.at[h, rows], send_sem=tok_send.at[slot, half],
            recv_sem=tok_recv.at[h, half], device_id=dev, device_id_type=MESH)

    def row_copy(slot, h, src):
        return pltpu.make_async_remote_copy(
            src_ref=src, dst_ref=X.at[h, 0:Y_ROWS], send_sem=tok_send.at[slot, 0],
            recv_sem=tok_recv.at[h, 0], device_id=id_y, device_id_type=MESH)

    def meta_copy(slot, h, dev):
        return pltpu.make_async_remote_copy(
            src_ref=M.at[h], dst_ref=M.at[h], send_sem=meta_send.at[slot],
            recv_sem=meta_recv.at[h], device_id=dev, device_id_type=MESH)

    @pl.when(c == 0)
    def _():
        tok_copy(0, 0, me, id_x, own=True).start()

    for half_no in range(2):
        tok_copy(2, half_no, me, id_p, own=True).start()
    for dx in range(2):
        for hc in range(2):
            X[home(1, dx, hc), Y_ROWS:, :] = jnp.zeros((num_tok - Y_ROWS, dim), BF16)

    earlier = (lax.broadcasted_iota(jnp.int32, (num_tok, num_tok), 0) < lax.broadcasted_iota(jnp.int32, (num_tok, num_tok), 1))
    earlier = jnp.where(earlier, 1.0, 0.0).astype(BF16)

    with jax.named_scope('load_wait'):
        for cp in loads:
            cp.wait()
        for j in range(per_dev):
            for cp in weight_copies(j):
                cp.start()
    with jax.named_scope('meta'):
        logits = lax.dot_general(Wr[...], X[me], (((1,), (1,)), ((), ())), preferred_element_type=F32)
        expert_id = lax.broadcasted_iota(jnp.int32, (num_exp, num_tok), 0)
        routed = expert_id == Rt[0:1, :]
        for j in range(1, Rt.shape[0]):
            routed = jnp.logical_or(routed, expert_id == Rt[j:j + 1, :])
        top = jnp.max(jnp.where(routed, logits, -jnp.inf), axis=0, keepdims=True)
        ex = jnp.where(routed, jnp.exp(jnp.where(routed, logits - top, 0.0)), 0.0)
        gates = ex / jnp.sum(ex, axis=0, keepdims=True)
        pos = jnp.dot(jnp.where(routed, 1.0, 0.0).astype(BF16), earlier, preferred_element_type=F32)
        M[me] = jnp.where(routed, jnp.where(pos < capacity, gates, DROPPED), UNROUTED)
    meta_copy(2, me, id_p).start()

    @pl.when(c == 0)
    def _():
        meta_copy(0, me, id_x).start()
        tok_copy(0, 1, me, id_x, own=True).start()

    slot_iota = lax.broadcasted_iota(jnp.int32, (capacity, num_tok), 0).astype(F32)
    rank_iota = lax.broadcasted_iota(jnp.int32, (cap, num_tok), 0).astype(F32)
    row_id = lax.broadcasted_iota(jnp.int32, (num_exp, num_tok), 0)
    in_row = jnp.logical_and(row_id >= o * half, row_id < o * half + half)

    row_iota = lax.broadcasted_iota(jnp.int32, (num_tok, num_tok), 0).astype(F32)

    def row_members(h):
        hit = jnp.logical_and(M[h] != UNROUTED, in_row)
        return jnp.max(jnp.where(hit, 1.0, 0.0), axis=0, keepdims=True)

    def plan(h):
        gates = [M[h, pl.ds(me * per_dev + j, 1), :] for j in range(per_dev)]
        members = row_members(h)
        marks = [jnp.where(g != UNROUTED, 1.0, 0.0) for g in gates] + [members]
        marks += [jnp.zeros_like(members)] * (8 - len(marks))
        before = jnp.dot(jnp.concatenate(marks, axis=0).astype(BF16), earlier, preferred_element_type=F32)
        slots = [jnp.where(g >= 0.0, before[j:j + 1], -1.0) for j, g in enumerate(gates)]
        rank = jnp.where(members > 0.5, before[per_dev:per_dev + 1], -1.0)
        return gates, slots, rank, members

    def compact(h, dst):
        others = 1.0 - row_members(h)
        before = jnp.dot(jnp.concatenate([others] * 8, axis=0).astype(BF16), earlier, preferred_element_type=F32)
        rank = jnp.where(others > 0.5, before[0:1], -1.0)
        sel = jnp.where(rank == row_iota[0:Y_ROWS], 1.0, 0.0).astype(BF16)
        dst[...] = jnp.dot(sel, X[h], preferred_element_type=F32).astype(BF16)

    with jax.named_scope('compact'):
        compact(me, Yo)

    @pl.when(c == 1)
    def _():
        meta_copy(0, me, id_y).start()
        row_copy(0, me, Yo).start()

    def d_copy(chip, k):
        return pltpu.make_async_remote_copy(
            src_ref=Pt.at[chip * 2 + 1 - c, k], dst_ref=Rd.at[chip, k], send_sem=d_send.at[chip, k],
            recv_sem=d_recv.at[chip, k], device_id=id_p, device_id_type=MESH)

    def x_copy(ho, k):
        return pltpu.make_async_remote_copy(
            src_ref=Pt.at[ho * 4 + (1 - x) * 2 + c, k], dst_ref=Rx.at[ho, k], send_sem=x_send.at[ho, k],
            recv_sem=x_recv.at[ho, k], device_id=id_x, device_id_type=MESH)

    def y_copy(k):
        return pltpu.make_async_remote_copy(
            src_ref=TS.at[k], dst_ref=TR.at[k], send_sem=y_send.at[k], recv_sem=y_recv.at[k],
            device_id=id_y, device_id_type=MESH)

    def rows_to_partner(slot, h):
        return pltpu.make_async_remote_copy(
            src_ref=X.at[h, 0:Y_ROWS], dst_ref=X.at[h, 0:Y_ROWS], send_sem=tok_send.at[slot, 0],
            recv_sem=tok_recv.at[h, 0], device_id=id_p, device_id_type=MESH)

    def at(cond, name, body):
        @pl.when(cond)
        def _():
            with jax.named_scope(name):
                body()

    def own_along_y():
        meta_copy(1, me, id_y).start()
        row_copy(1, me, Yo).start()

    def own_along_x():
        tok_copy(1, 0, me, id_x, own=True).start()
        meta_copy(1, me, id_x).start()
        tok_copy(1, 1, me, id_x, own=True).start()

    def forward_x():
        compact(h_x, Yf)
        meta_copy(6, h_x, id_y).start()
        row_copy(6, h_x, Yf).start()

    def x_arrived(half):
        if half == 0:
            meta_copy(3, h_x, id_p).wait_recv()
            meta_copy(3, h_x, id_p).start()
        tok_copy(3, half, h_x, id_p).wait_recv()
        tok_copy(3, half, h_x, id_p).start()
        if half == 1:
            forward_x()

    def rows_arrived(slot, h):
        meta_copy(slot, h, id_p).wait_recv()
        meta_copy(slot, h, id_p).start()
        rows_to_partner(slot, h).wait_recv()
        rows_to_partner(slot, h).start()

    def finish(ho, last):
        chip = ho * 2 + 1 - x
        for k in range(blocks):
            d_copy(chip, k).wait_recv()
            Pt[chip * 2 + c, k] = Pt[chip * 2 + c, k] + Rd[chip, k]
            if last or k < blocks - 1:
                x_copy(ho, k).start()
        if last:
            x_copy(o, blocks - 1).start()

    Over[...] = jnp.zeros_like(Over)
    token_id = lax.broadcasted_iota(jnp.int32, (1, num_tok), 1).astype(F32)

    def place(n):
        dy, dx, hc = bit(DY_BITS, n), bit(DX_BITS, n), bit(HC_BITS, n)
        return home(dy, dx, hc), dy, hc

    def out_slot(n):
        return jnp.where(n < 2, 4 + n, lax.rem(n + 2, 4))

    def combine(n, send):
        h, dy, hc = place(n)
        outs = out_slot(n)
        with jax.named_scope('combine'):
            gates, slots = Pg[n], Ps[n]
            spread = jnp.concatenate([jnp.where(slots[j:j + 1] == slot_iota, gates[j:j + 1], 0.0) for j in range(per_dev)], axis=0)
            where_to = jnp.where(slots[per_dev:per_dev + 1] == rank_iota, 1.0, 0.0).astype(BF16)
            parts = []
            for _ in range(3):
                parts.append(spread.astype(BF16))
                spread = spread - parts[-1].astype(F32)
            tiles = [p[0:TILE] for p in parts] + [jnp.concatenate([p[TILE:] for p in parts], axis=0)]
            weights = [lax.dot_general(where_to, t, (((1,), (1,)), ((), ())), preferred_element_type=F32).astype(BF16)
                       for t in tiles]
            for k in range(blocks):
                cols = slice(k * NBLK, (k + 1) * NBLK)
                acc = jnp.dot(weights[3], Ob[outs, TILE:, cols], preferred_element_type=F32)
                for w in weights[:3]:
                    acc += jnp.dot(w, Ob[outs, 0:TILE, cols], preferred_element_type=F32)
                Pt[h, k] = acc
                if send and k + 1 in SEND_AFTER:
                    for done in range(max([0] + [b for b in SEND_AFTER if b <= k]), k + 1):
                        d_copy(h // 2, done).start()

    def step(i, carry):
        places = [place(2 * i), place(2 * i + 1)]
        first_other = jnp.where(places[0][2] == c, 1, 0)
        other, other_dy, _ = place(2 * i + first_other)
        with jax.named_scope('wait_meta'):
            meta_copy(2, other, id_p).wait_recv()

        with jax.named_scope('plan'):
            for n, (h, dy, hc) in enumerate(places):
                gates, slots, rank, members = plan(h)
                count = jnp.sum(members, axis=1, keepdims=True)
                Over[...] = jnp.maximum(Over[...], jnp.maximum(count, num_tok - count))
                pad = [jnp.full_like(rank, -1.0)] * (8 - per_dev - 1)
                stored = jnp.concatenate(slots + [rank] + pad, axis=0)
                Ps[2 * i + n] = stored
                Pg[2 * i + n] = jnp.concatenate(gates + [rank] + pad, axis=0)
                key = jnp.where(dy == 1, rank, token_id)
                held = lax.dot_general((stored + 1.0).astype(BF16), jnp.where(key == row_iota, 1.0, 0.0).astype(BF16),
                                       (((1,), (1,)), ((), ())), preferred_element_type=F32) - 1.0
                for j in range(per_dev):
                    Pick[n, j * capacity:(j + 1) * capacity, :] = jnp.where(held[j:j + 1] == slot_iota, 1.0, 0.0).astype(BF16)

        @pl.when(other_dy == 0)
        def _():
            with jax.named_scope('wait_other'):
                for half_no in range(2):
                    tok_copy(2, half_no, other, id_p).wait_recv()

        at(other_dy == 1, 'wait_rows', lambda: rows_to_partner(2, other).wait_recv())

        with jax.named_scope('fill'):
            for n, (h, dy, hc) in enumerate(places):
                for k in range(blocks):
                    cols = slice(k * NBLK, (k + 1) * NBLK)
                    rows = jnp.dot(Pick[n], X[h, :, cols], preferred_element_type=F32).astype(BF16)
                    for j in range(per_dev):
                        Xs[j, n * capacity:(n + 1) * capacity, cols] = rows[j * capacity:(j + 1) * capacity]

        @pl.when(i == 0)
        def _():
            for j in range(per_dev):
                for cp in weight_copies(j):
                    cp.wait()

            @pl.when(c == 0)
            def _():
                own_along_y()
                with jax.named_scope('wait_hx0a'):
                    x_arrived(0)

        with jax.named_scope('experts'):
            for j in range(per_dev):
                if j == 3:
                    at(jnp.logical_and(i == 0, c == 1), 'own_along_x', own_along_x)
                rows = Xs[j]
                act = jnp.dot(rows, Wg[j], preferred_element_type=F32)
                lin = jnp.dot(rows, Wu[j], preferred_element_type=F32)
                hidden = (jax.nn.silu(act) * lin).astype(BF16)
                res = jnp.dot(hidden, Wd[j], preferred_element_type=F32).astype(BF16)
                for n in range(2):
                    part = res[n * capacity:(n + 1) * capacity]
                    slot = out_slot(2 * i + n)
                    Ob[slot, j * capacity:(j + 1) * capacity, :] = part
                    if (j + 1) * capacity > TILE:
                        for copy in (1, 2):
                            lo = j * capacity + copy * (per_dev * capacity - TILE)
                            Ob[slot, lo:lo + capacity, :] = part

        at(jnp.logical_and(i == 0, c == 0), 'wait_hx0b', lambda: x_arrived(1))
        at(jnp.logical_and(i == 0, c == 1), 'wait_hy1', lambda: rows_arrived(4, h_y))
        at(jnp.logical_and(i == 1, c == 1), 'wait_hx1a', lambda: x_arrived(0))

        def pair(q, carry):
            p = lax.rem(i + q, 4)
            non = jnp.where(place(2 * p)[2] == c, 1, 0)
            combine(2 * p + non, True)
            at(jnp.logical_and(i == 1, c == 0), 'wait_hy0', lambda: rows_arrived(4, h_y))
            at(jnp.logical_and(i == 1, c == 1), 'wait_hx1b', lambda: x_arrived(1))
            at(jnp.logical_and(i == 2, c == 0), 'wait_hd0', lambda: rows_arrived(5, h_d))
            combine(2 * p + 1 - non, False)
            at(jnp.logical_and(i == 1, c == 0), 'finish_x0', lambda: finish(o, False))
            at(jnp.logical_and(i == 2, c == 1), 'finish_x1', lambda: finish(o, False))
            at(jnp.logical_and(i == 2, c == 1), 'wait_hd1', lambda: rows_arrived(5, h_d))
            at(jnp.logical_and(i == 3, q == 0), 'finish_d', lambda: finish(1 - o, True))
            return carry

        lax.fori_loop(0, jnp.where(i == 0, 0, jnp.where(i == 3, 2, 1)), pair, 0)
        return carry

    lax.fori_loop(0, 4, step, 0)
    flag_ref[0, 0] = jnp.where(jnp.max(Over[...]) > cap, 1, 0)

    def total(ho, k):
        chip = ho * 2 + x
        with jax.named_scope('wait_x'):
            x_copy(ho, k).wait_recv()
        d_copy(chip, k).wait_recv()
        return (Pt[chip * 2 + c, k] + Rd[chip, k] + Rx[ho, k]).astype(BF16)

    members = row_members(me)
    marks = jnp.concatenate([members, 1.0 - members] + [jnp.zeros_like(members)] * 6, axis=0)
    before = jnp.dot(marks.astype(BF16), earlier, preferred_element_type=F32)
    ranks = jnp.where(marks > 0.5, before, -1.0)
    ranks = jnp.transpose(jnp.concatenate([ranks] * (LANES // 8), axis=0))
    cap_iota = lax.broadcasted_iota(jnp.int32, (num_tok, cap), 1).astype(F32)
    take_here = jnp.where(ranks[:, 0:1] == cap_iota, 1.0, 0.0).astype(BF16)
    take_there = jnp.where(ranks[:, 1:2] == cap_iota, 1.0, 0.0).astype(BF16)

    def emit(k):
        with jax.named_scope('wait_y'):
            y_copy(k).wait_recv()
        acc = jnp.dot(take_here, TL[k], preferred_element_type=F32)
        acc += jnp.dot(take_there, TR[k], preferred_element_type=F32)
        out_ref[:, k * NBLK:(k + 1) * NBLK] = acc.astype(BF16)

    for k in range(blocks - 1):
        TL[k] = total(o, k)
    for k in range(blocks):
        TS[k] = total(1 - o, k)
        y_copy(k).start()
        if k > 0:
            emit(k - 1)
    TL[blocks - 1] = total(o, blocks - 1)
    emit(blocks - 1)

    for half_no in range(2):
        @pl.when(c == 0)
        def _():
            tok_copy(0, half_no, me, id_x, own=True).wait_send()

        @pl.when(c == 1)
        def _():
            tok_copy(1, half_no, me, id_x, own=True).wait_send()

        tok_copy(2, half_no, me, id_p, own=True).wait_send()
        tok_copy(3, half_no, h_x, id_p).wait_send()

    @pl.when(c == 0)
    def _():
        row_copy(1, me, Yo).wait_send()

    @pl.when(c == 1)
    def _():
        row_copy(0, me, Yo).wait_send()

    rows_to_partner(4, h_y).wait_send()
    rows_to_partner(5, h_d).wait_send()
    row_copy(6, h_x, Yf).wait_send()
    for slot in range(7):
        meta_copy(slot, me, id_p).wait_send()
    for k in range(blocks):
        for chip in range(4):
            d_copy(chip, k).wait_send()
        for ho in range(2):
            x_copy(ho, k).wait_send()
        y_copy(k).wait_send()


def solution(mesh):
    outer_size = mesh.shape['outer']
    group_size = mesh.shape['expert']
    row_spec = P(('data', 'outer', 'expert'), None)
    weight_spec = P(('outer', 'expert'), None, None)

    def per_device(tokens, w_router, routes, w_gate, w_up, w_down):
        tok_count, top_k = routes.shape
        dim = tokens.shape[1]
        num_exp = w_router.shape[1]
        per_dev, _, ffn = w_gate.shape
        capacity = (5 * tok_count * top_k + 4 * num_exp - 1) // (4 * num_exp)
        homes = outer_size * group_size
        cap = ROWS_CAP
        blocks = dim // NBLK
        hbm = pl.BlockSpec(memory_space=pl.ANY)
        dma = pltpu.SemaphoreType.DMA

        def body(*refs):
            moe_kernel(capacity, *refs)

        fast, flag = pl.pallas_call(
            body,
            out_shape=(pltpu.VMEM((tok_count, dim), BF16), jax.ShapeDtypeStruct((1, 1), jnp.int32)),
            in_specs=[hbm] * 6,
            out_specs=(pl.BlockSpec(memory_space=pltpu.VMEM), pl.BlockSpec(memory_space=pltpu.SMEM)),
            scratch_shapes=[
                pltpu.VMEM((homes, tok_count, dim), BF16),
                pltpu.VMEM((homes, num_exp, tok_count), F32),
                pltpu.VMEM((Y_ROWS, dim), BF16),
                pltpu.VMEM((Y_ROWS, dim), BF16),
                pltpu.VMEM((top_k, tok_count), jnp.int32),
                pltpu.VMEM((num_exp, dim), BF16),
                pltpu.VMEM((per_dev, dim, ffn), BF16),
                pltpu.VMEM((per_dev, dim, ffn), BF16),
                pltpu.VMEM((per_dev, ffn, dim), BF16),
                pltpu.VMEM((per_dev, 2 * capacity, dim), BF16),
                pltpu.VMEM((6, TILE + 3 * (per_dev * capacity - TILE), dim), BF16),
                pltpu.VMEM((homes, blocks, cap, NBLK), F32),
                pltpu.VMEM((homes // 2, blocks, cap, NBLK), F32),
                pltpu.VMEM((2, blocks, cap, NBLK), F32),
                pltpu.VMEM((blocks, cap, NBLK), BF16),
                pltpu.VMEM((blocks, cap, NBLK), BF16),
                pltpu.VMEM((blocks, cap, NBLK), BF16),
                pltpu.VMEM((8, LANES), F32),
                pltpu.VMEM((homes, 8, tok_count), F32),
                pltpu.VMEM((homes, 8, tok_count), F32),
                pltpu.VMEM((2, per_dev * capacity, tok_count), BF16),
                dma((7, 2)), dma((homes, 2)), dma((7,)), dma((homes,)),
                dma((homes // 2, blocks)), dma((homes // 2, blocks)),
                dma((2, blocks)), dma((2, blocks)), dma((blocks,)), dma((blocks,)),
                dma((3, per_dev)), dma((3,)),
            ],
            compiler_params=pltpu.CompilerParams(collective_id=0, has_side_effects=True, vmem_limit_bytes=66_000_000),
            name='moe',
        )(tokens, routes.T, w_router.T, w_gate, w_up, w_down)

        def slow():
            return plain_layer(tokens, w_router, routes, w_gate, w_up, w_down, outer_size, group_size, capacity)

        return lax.switch(flag[0, 0], [lambda: fast, slow])

    return jax.shard_map(per_device, mesh=mesh, in_specs=(row_spec, P(), row_spec, weight_spec, weight_spec, weight_spec), out_specs=row_spec, check_vma=False)
```
